16 devices in a mesh: outer: 2 (over z), middle: 2 (over y), inner: 4 (over x, core).
Axes of the slice: x: 2, y: 2, z: 2, core: 2. Of those that a mesh axis runs over, the one named last changes fastest.
Arguments:
- g_embed: float32 [16, 2048, 768], P(('outer', 'middle', 'inner'))
- g_attn: float32 [16, 2, 768, 3072], P(('outer', 'middle', 'inner'))
- g_ffn_in: float32 [16, 2, 768, 3072], P(('outer', 'middle', 'inner'))
- g_ffn_out: float32 [16, 2, 3072, 768], P(('outer', 'middle', 'inner'))
- g_vec: float32 [16, 2, 9984], P(('outer', 'middle', 'inner'))
- m_flat: float32 [15748608], P(('outer', 'middle', 'inner'))
- v_flat: float32 [15748608], P(('outer', 'middle', 'inner'))
- w_flat: float32 [15748608], P(('outer', 'middle', 'inner'))
Outputs:
- output 1: float32 [15748608], P(('outer', 'middle', 'inner'))
- output 2: float32 [15748608], P(('outer', 'middle', 'inner'))
- output 3: float32 [15748608], P(('outer', 'middle', 'inner'))
- output 4: bfloat16 [2048, 768], replicated
- output 5: bfloat16 [2, 768, 3072], replicated
- output 6: bfloat16 [2, 768, 3072], replicated
- output 7: bfloat16 [2, 3072, 768], replicated
- output 8: bfloat16 [2, 9984], replicated
- output 9: bfloat16 [16, 1968576], P(('outer', 'middle', 'inner'))
All inputs are finite; a program needn't handle non-finite values.
Results may differ from the reference program's by a relative error of at most 0.001.
Values are sent between devices in bfloat16 or wider.
A program may use at most 1 GiB of HBM per device.

```python
import math
import jax
import jax.numpy as jnp

DEVICES = 16
VOCAB_ROWS = 2048
D = 768
FF = 3072
LAYERS = 2
ADAM_STEP = 3

ADAM_BETA1 = 0.9
ADAM_BETA2 = 0.98
ADAM_EPS = 1e-9
LEARN_RATE = 0.05
NUM_CHIPS = DEVICES // 2
VEC_WIDTH = 9 * D + FF
TENSOR_SHAPES = ((VOCAB_ROWS, D), (LAYERS, D, 4 * D), (LAYERS, D, FF), (LAYERS, FF, D), (LAYERS, VEC_WIDTH))
PARAM_COUNT = sum(math.prod(shape) for shape in TENSOR_SHAPES)


def draw_gradient(gen_key, shape):
    common_key, chip_key, core_key = jax.random.split(gen_key, 3)
    common = jax.random.normal(common_key, shape, jnp.float32)
    per_chip = jax.random.normal(chip_key, (NUM_CHIPS,) + shape, jnp.float32)
    per_core = jax.random.normal(core_key, (DEVICES,) + shape, jnp.float32)
    return common[None] + jnp.repeat(per_chip, 2, axis=0) + 0.25 * per_core


def setup_inputs(seed: int = 0) -> dict:
    key_list = jax.random.split(jax.random.key(seed), 8)
    return {
        'g_embed': draw_gradient(key_list[0], TENSOR_SHAPES[0]),
        'g_attn': draw_gradient(key_list[1], TENSOR_SHAPES[1]),
        'g_ffn_in': draw_gradient(key_list[2], TENSOR_SHAPES[2]),
        'g_ffn_out': draw_gradient(key_list[3], TENSOR_SHAPES[3]),
        'g_vec': draw_gradient(key_list[4], TENSOR_SHAPES[4]),
        'm_flat': 0.3 * jax.random.normal(key_list[5], (PARAM_COUNT,), jnp.float32),
        'v_flat': 0.1 * (0.5 + jax.random.uniform(key_list[6], (PARAM_COUNT,), jnp.float32)),
        'w_flat': jax.random.normal(key_list[7], (PARAM_COUNT,), jnp.float32),
    }


def adam_update(grad_mean, m_old, v_old, w_old):
    m_new = ADAM_BETA1 * m_old + (1.0 - ADAM_BETA1) * grad_mean
    v_new = ADAM_BETA2 * v_old + (1.0 - ADAM_BETA2) * (grad_mean * grad_mean)
    m_hat = m_new / (1.0 - ADAM_BETA1 ** ADAM_STEP)
    v_hat = v_new / (1.0 - ADAM_BETA2 ** ADAM_STEP)
    w_new = w_old - LEARN_RATE * m_hat / (jnp.sqrt(v_hat) + ADAM_EPS)
    return m_new, v_new, w_new


def split_tensors(flat_values, shape_list):
    pieces = []
    offset = 0
    for shape in shape_list:
        count = math.prod(shape)
        pieces.append(flat_values[offset:offset + count].reshape(shape))
        offset += count
    return pieces


def chip_blocks(w_tensors, num_chips):
    blocks = [w_tensors[0].reshape(num_chips, -1)]
    for tensor in w_tensors[1:]:
        layer_count = tensor.shape[0]
        blocks.append(jnp.swapaxes(tensor.reshape(layer_count, num_chips, -1), 0, 1).reshape(num_chips, -1))
    return jnp.concatenate(blocks, axis=1)


def reference(g_embed, g_attn, g_ffn_in, g_ffn_out, g_vec, m_flat, v_flat, w_flat):
    grad_list = (g_embed, g_attn, g_ffn_in, g_ffn_out, g_vec)
    grad_mean = jnp.concatenate([jnp.sum(gradient, axis=0).reshape(-1) for gradient in grad_list]) / DEVICES
    m_new, v_new, w_new = adam_update(grad_mean, m_flat, v_flat, w_flat)
    w_tensors = split_tensors(w_new.astype(jnp.bfloat16), TENSOR_SHAPES)
    w_chip = jnp.repeat(chip_blocks(w_tensors, NUM_CHIPS), 2, axis=0)
    return (m_new, v_new, w_new, w_tensors[0], w_tensors[1], w_tensors[2], w_tensors[3], w_tensors[4], w_chip)
```

```python
import jax
import jax.numpy as jnp
from jax import lax
from jax.experimental import pallas as pl
from jax.experimental.pallas import tpu as pltpu
from jax.sharding import PartitionSpec as P

MESH_AXES = ('outer', 'middle', 'inner')
ADAM_BETA1 = 0.9
ADAM_BETA2 = 0.98
ADAM_EPS = 1e-9
LEARN_RATE = 0.05
ADAM_STEP = 3

TILE = (8, 128)
LANES = TILE[1]
TILE_SIZE = 1024
ROUNDS = 10
TILES = 96
SLOTS = ((0, 48, 0, 0), (1, 24, 48, 384), (2, 24, 72, 576))
BLOCKS = 8 * TILES
TENSOR_GROUPS = (0, 16, 64, 112, 160)
ROWS = 768
FLAT = ROUNDS * ROWS * 128
SHARD = 984288
STEP = SHARD - FLAT
BTAIL = 16 * STEP
BROWS = 160
BPAD = BROWS - BTAIL // 128
RAW_ROWS = ROWS + BROWS
OUT_ROWS = ROUNDS * ROWS + 2 * BROWS
NACC = 5
STAGES = ROUNDS + 6
MESH = pl.DeviceIdType.MESH


def loop(count, body, **options):
    lax.fori_loop(0, count, lambda i, carry: (body(i), carry)[1], None, **options)


def top(n):
    return pl.ds(0, n)


def device_number():
    return (lax.axis_index('outer') * 2 + lax.axis_index('middle')) * 4 + lax.axis_index('inner')


def mesh_id(d):
    return (d // 8, (d // 4) % 2, d % 4)


def adam_update(grad_mean, m_old, v_old, w_old):
    m_new = ADAM_BETA1 * m_old + (1.0 - ADAM_BETA1) * grad_mean
    v_new = ADAM_BETA2 * v_old + (1.0 - ADAM_BETA2) * (grad_mean * grad_mean)
    m_hat = m_new / (1.0 - ADAM_BETA1 ** ADAM_STEP)
    v_hat = v_new / (1.0 - ADAM_BETA2 ** ADAM_STEP)
    w_new = w_old - LEARN_RATE * m_hat / (jnp.sqrt(v_hat) + ADAM_EPS)
    return m_new, v_new, w_new


def axis_weights(a):
    return ((a - 1) * (a - 2)) // 2, a * (2 - a), (a * (a - 1)) // 2


def pick(values, a):
    e0, e1, e2 = axis_weights(a)
    return values[0] * e0 + values[1] * e1 + values[2] * e2


def chip_bits(d):
    return (d // 2) % 2, (d // 4) % 2, d // 8


def comm_kernel(ge, ga, gf, gh, gb, m1, v1, w1, mvwb,
                wst, m_out, v_out, w_out, wb_out,
                acc, sib, l1, l2, l3, flat_in, raw, mv, flat_out, heads, wt, bs, bl, bout, wbs, wbl,
                own_sem, sib_send, sib_recv, rs_send, rs_recv, ag_send, ag_recv, fw_send, fw_recv,
                loc_sem, in_sem, out_sem, b_send, b_recv, end_sem, head_sem, free_sem):
    me = device_number()
    core = me % 2
    mate = me + 1 - 2 * core
    bits = chip_bits(me)
    deltas = tuple(m * (1 - 2 * b) for m, b in zip((2, 4, 8), bits))
    partners = (mate,) + tuple(me + d for d in deltas)
    grads = (ge, ga, gf, gh)
    olds = tuple(enumerate((m1, v1, w1)))
    outs = tuple(enumerate((m_out, v_out, w_out)))
    shift_rows = (STEP * me) // LANES
    shift_lanes = (STEP * me) % LANES
    back_lanes = (LANES - shift_lanes) % LANES
    lane = lax.broadcasted_iota(jnp.int32, TILE, 1)

    barrier = pltpu.get_barrier_semaphore()
    for other in partners + ((me + 1) % 16, (me + 15) % 16):
        pl.semaphore_signal(barrier, inc=1, device_id=mesh_id(other), device_id_type=MESH)
    pl.semaphore_wait(barrier, 6)

    def remote(src, dst, ssem, rsem, dev):
        return pltpu.make_async_remote_copy(src_ref=src, dst_ref=dst, send_sem=ssem, recv_sem=rsem,
                                            device_id=mesh_id(dev), device_id_type=MESH)

    def turned(r):
        steps = [pick(deltas, lax.rem(r + j, 3)) for j in range(3)]
        return [[steps[(t + j) % 3] for j in range(3)] for t in range(3)]

    def any_tiles(n):
        return ga.at[top(n)]

    def rs_wait(r, j):
        half = acc.at[0, top(BLOCKS // 2 >> j)]
        remote(half, half, rs_send.at[r, j], rs_recv.at[r, 0, j], mate).wait_send()

    def load_round(r):
        a = r % NACC
        b = r % 2

        steps = turned(r)

        def body(back):
            rel = 7 - back
            betas = (rel // 4, (rel // 2) % 2, rel % 2)
            for t, n, first, base in SLOTS:
                d = me + sum(beta * step for beta, step in zip(betas, steps[t]))
                at = pl.ds(base + rel * n, n)
                for other in (False, True):
                    group = ROUNDS * (d + (mate - me if other else 0)) + r
                    for ref, lo, hi in zip(grads, TENSOR_GROUPS, TENSOR_GROUPS[1:]):
                        @pl.when((group >= lo) & (group < hi))
                        def _(ref=ref, lo=lo, other=other, group=group):
                            src = ref.at[pl.ds((group - lo) * TILES + first, n)]
                            if other:
                                remote(src, sib.at[b, at], sib_send.at[b], sib_recv.at[b, rel // 4], mate).start()
                            else:
                                pltpu.make_async_copy(src, acc.at[a, at], own_sem.at[a, rel // 4]).start()

        loop(8, body)

    def add_range(dst, src, n):
        def body(i):
            at = pl.ds(i * 8, 8)
            dst[at] = dst[at] + src[at]

        loop(n // 8, body)

    def when_round(r):
        return pl.when((r >= 0) & (r < ROUNDS))

    def old_copy(ref, r, i, skip):
        n = (RAW_ROWS - skip) * LANES
        at = ((r % 2 * 3 + i) * RAW_ROWS + skip) * LANES
        return pltpu.make_async_copy(ref.at[pl.ds((r * ROWS - BROWS + skip) * LANES, n)], flat_in.at[pl.ds(at, n)],
                                     in_sem.at[r % 2])

    def old_rows(r, skip):
        for i, ref in olds:
            old_copy(ref, r, i, skip).wait()

        def body(k):
            row = skip + k * 8
            for i, ref in olds:
                at = ((r % 2 * 3 + i) * RAW_ROWS + row) * LANES
                raw[i, pl.ds(row, 8), :] = flat_in[pl.ds(pl.multiple_of(at, TILE_SIZE), TILE_SIZE)].reshape(TILE)

        loop((RAW_ROWS - skip) // 8, body)

    def out_copy(ref, b, i, r, n):
        at = pl.multiple_of((r * ROWS + BROWS - 1 - shift_rows) * LANES, LANES)
        return pltpu.make_async_copy(flat_out.at[pl.ds((b * 3 + i) * ROWS * LANES, n * LANES)], ref.at[pl.ds(at, n * LANES)],
                                     out_sem.at[b])

    def put_out(b, r, n):
        def body(k):
            for i, ref in outs:
                low = pltpu.roll(mv[i, pl.ds(k * 8 + 7, 8), :], back_lanes, 1)
                high = pltpu.roll(mv[i, pl.ds(k * 8 + 8, 8), :], back_lanes, 1)
                at = ((b * 3 + i) * ROWS + k * 8) * LANES
                both = jnp.where(lane < LANES - shift_lanes, low, high)
                flat_out[pl.ds(pl.multiple_of(at, TILE_SIZE), TILE_SIZE)] = both.reshape(TILE_SIZE)

        loop(n // 8, body)
        for i, ref in outs:
            out_copy(ref, b, i, r, n).start()

    def wait_out(b, n):
        for i, ref in outs:
            out_copy(ref, b, i, 0, n).wait()

    load_round(0)

    @pl.when(me < 15)
    def _():
        remote(mvwb, raw.at[:, top(BROWS)], end_sem.at[0], end_sem.at[1], me + 1).start()

    def stage(s):
        nxt = s + 1

        @pl.when((nxt >= NACC) & (nxt < ROUNDS))
        def _():
            for j in range(3):
                rs_wait(nxt - NACC, j)

        @pl.when((nxt >= 2) & (nxt < ROUNDS))
        def _():
            remote(any_tiles(BLOCKS), sib.at[0], sib_send.at[nxt % 2], sib_recv.at[0, 0], mate).wait_send()
            pl.semaphore_wait(free_sem, 1)

        @pl.when(nxt < ROUNDS)
        def _():
            load_round(nxt)

        @pl.when(s == 2)
        def _():
            for i, ref in olds:
                old_copy(ref, 0, i, BROWS).start()

        @pl.when((s > 2) & (s < ROUNDS + 2))
        def _():
            for i, ref in olds:
                old_copy(ref, s - 2, i, 0).start()

        @when_round(s)
        def _():
            r, a, b = s, s % NACC, s % 2
            steps = turned(r)

            def loaded(part):
                src, half = any_tiles(BLOCKS // 2), top(BLOCKS // 2)
                pltpu.make_async_copy(src, acc.at[a, half], own_sem.at[a, part]).wait()
                remote(src, sib.at[b, half], sib_send.at[b], sib_recv.at[b, part], mate).wait_recv()

            loaded(1)
            for t, n, first, base in SLOTS:
                hi = pl.ds(base + 4 * n, 4 * n)
                add_range(acc.at[a, hi], sib.at[b, hi], 4 * n)
            for t, n, first, base in SLOTS:
                remote(acc.at[a, pl.ds(base + 4 * n, 4 * n)], l1.at[r, pl.ds(base // 2, 4 * n)],
                       rs_send.at[r, 0], rs_recv.at[r, t, 0], me + steps[t][0]).start()
            loaded(0)
            for t, n, first, base in SLOTS:
                lo = pl.ds(base, 4 * n)
                add_range(acc.at[a, lo], sib.at[b, lo], 4 * n)

            @pl.when(r + 2 < ROUNDS)
            def _():
                pl.semaphore_signal(free_sem, inc=1, device_id=mesh_id(mate), device_id_type=MESH)

        for j, land, out in ((1, l1, l2), (2, l2, l3)):
            @when_round(s - j)
            def _(j=j, land=land, out=out):
                r = s - j
                a = r % NACC
                keep = 4 >> j
                steps = turned(r)
                for t, n, first, base in SLOTS:
                    here = land.at[r, pl.ds(base >> j, 2 * keep * n)]
                    remote(here, here, rs_send.at[r, j - 1], rs_recv.at[r, t, j - 1], mate).wait_recv()
                    add_range(acc.at[a, pl.ds(base + keep * n, keep * n)],
                              land.at[r, pl.ds((base >> j) + keep * n, keep * n)], keep * n)
                for t, n, first, base in SLOTS:
                    remote(acc.at[a, pl.ds(base + keep * n, keep * n)], out.at[r, pl.ds(base >> (j + 1), keep * n)],
                           rs_send.at[r, j], rs_recv.at[r, t, j], me + steps[t][j]).start()
                for t, n, first, base in SLOTS:
                    add_range(acc.at[a, pl.ds(base, keep * n)], land.at[r, pl.ds(base >> j, keep * n)], keep * n)

        @when_round(s - 3)
        def _():
            r = s - 3
            a, b = r % NACC, r % 2

            @pl.when(r == 0)
            def _():
                old_rows(0, BROWS)

            @pl.when((r == 0) & (me > 0))
            def _():
                remote(mvwb, raw.at[:, top(BROWS)], end_sem.at[0], end_sem.at[1], mate).wait_recv()

            @pl.when(r > 0)
            def _():
                old_rows(r, 0)

            @pl.when((r == 1) & (me > 0))
            def _():
                remote(mv.at[:, pl.ds(8, BROWS)], heads, head_sem.at[0], head_sem.at[1], mate).wait_send()

            for i, ref in outs:
                mv[i, pl.ds(7, 1), :] = mv[i, pl.ds(ROWS + 7, 1), :]
            for t, n, first, base in SLOTS:
                here = l3.at[r, pl.ds(first, n)]
                remote(here, here, rs_send.at[r, 2], rs_recv.at[r, t, 2], mate).wait_recv()
            steps = turned(r)
            group = ROUNDS * me + r
            wide = (group >= TENSOR_GROUPS[1]) & (group < TENSOR_GROUPS[3])

            def adam_pass(stride):
                for t, n, first, base in SLOTS:
                    def body(u, first=first, base=base):
                        unit = first // 6 + u
                        if stride == 6:
                            row = unit * 48
                        else:
                            row = (unit // 4) * 192 + (unit % 4) * 6
                        for j in range(6):
                            old = []
                            for i, ref in olds:
                                at = row + j + BROWS - shift_rows
                                here = pltpu.roll(raw[i, pl.ds(at, 8, stride=stride), :], shift_lanes, 1)
                                prev = pltpu.roll(raw[i, pl.ds(at - 1, 8, stride=stride), :], shift_lanes, 1)
                                old.append(jnp.where(lane >= shift_lanes, here, prev))
                            tile = acc[a, base + u * 6 + j] + l3[r, unit * 6 + j]
                            new = adam_update(tile * (1.0 / 16.0), *old)
                            for i, ref in olds:
                                mv[i, pl.ds(row + j + 8, 8, stride=stride), :] = new[i]
                            wt[r, unit * 6 + j] = new[2].astype(jnp.bfloat16)

                    loop(n // 6, body)

            @pl.when(wide)
            def _():
                adam_pass(24)

            @pl.when(jnp.logical_not(wide))
            def _():
                adam_pass(6)

            for t, n, first, base in SLOTS:
                src = wt.at[r, pl.ds(first, n)]
                remote(src, wst.at[core, r, pl.ds(base + n, n)], ag_send.at[r, 0], ag_recv.at[r, t, 0],
                       me + steps[t][0]).start()
                remote(src, wst.at[core, r, pl.ds(base, n)], fw_send.at[r, 0], fw_recv.at[r, 0], mate).start()
                pltpu.make_async_copy(src, wst.at[core, r, pl.ds(base, n)], loc_sem.at[r]).start()

            @pl.when((r == 0) & (me > 0))
            def _():
                remote(mv.at[:, pl.ds(8, BROWS)], heads, head_sem.at[0], head_sem.at[1], me - 1).start()

            @pl.when(r >= 2)
            def _():
                wait_out(b, ROWS)

            put_out(b, r, ROWS)

        @pl.when((s == ROUNDS + 3) & (me < 15))
        def _():
            remote(mvwb, raw.at[:, top(BROWS)], end_sem.at[0], end_sem.at[1], mate).wait_send()
            remote(mv.at[:, pl.ds(8, BROWS)], heads, head_sem.at[0], head_sem.at[1], mate).wait_recv()

        @pl.when(s == ROUNDS + 3)
        def _():
            wait_out(0, ROWS)
            for i, ref in outs:
                mv[i, pl.ds(7, 1), :] = mv[i, pl.ds(ROWS + 7, 1), :]
                mv[i, pl.ds(8, BROWS), :] = heads[i]
            put_out(0, ROUNDS, BROWS)

        for j in (1, 2, 3):
            @when_round(s - 3 - j)
            def _(j=j):
                r = s - 3 - j
                got = 1 << (j - 1)
                steps = turned(r)
                if j == 1:
                    pltpu.make_async_copy(wt.at[r], wst.at[core, r, top(TILES)], loc_sem.at[r]).wait()
                for t, n, first, base in SLOTS:
                    here = wst.at[core, r, pl.ds(base + got * n, got * n)]
                    remote(here, here, ag_send.at[r, j - 1], ag_recv.at[r, t, j - 1], mate).wait_recv()
                    if j < 3:
                        remote(wst.at[core, r, pl.ds(base, 2 * got * n)],
                               wst.at[core, r, pl.ds(base + 2 * got * n, 2 * got * n)],
                               ag_send.at[r, j], ag_recv.at[r, t, j], me + steps[t][j]).start()
                    remote(here, here, fw_send.at[r, j], fw_recv.at[r, j], mate).start()

        for j in range(9):
            @pl.when(s == j)
            def _(j=j):
                if j > 0:
                    i = j - 1
                    land = bl.at[i] if i < 4 else wbl.at[i - 4]
                    remote(land, land, b_send.at[i], b_recv.at[i], mate).wait_recv()
                if j < 4:
                    src = gb
                    if j > 0:
                        src = bs.at[j - 1]
                        src[...] = (gb[...] if j == 1 else bs[j - 2]) + bl[j - 1]
                    remote(src, bl.at[j], b_send.at[j], b_recv.at[j], partners[j]).start()
                elif j < 8:
                    if j == 4:
                        new = adam_update((bs[2] + bl[3]) * (1.0 / 16.0), mvwb[0], mvwb[1], mvwb[2])
                        for i, ref in outs:
                            bout[i] = new[i]
                        keep = jnp.broadcast_to(me, (BROWS, LANES)) == 15
                        wbs[0] = jnp.where(keep, new[2], 0.0).astype(jnp.bfloat16)

                        @pl.when(me == 15)
                        def _():
                            for i, ref in outs:
                                heads[i, top(BROWS - BPAD), :] = bout[i, pl.ds(BPAD, BROWS - BPAD), :]
                    else:
                        wbs[j - 4] = wbs[j - 5] + wbl[j - 5]
                    remote(wbs.at[j - 4], wbl.at[j - 4], b_send.at[j], b_recv.at[j], partners[j - 4]).start()
                else:
                    wb_out[...] = wbs[3] + wbl[3]

    loop(STAGES, stage)

    for j in range(4):
        remote(gb, bl.at[j], b_send.at[j], b_recv.at[j], mate).wait_send()
        remote(wbs.at[j], wbl.at[j], b_send.at[4 + j], b_recv.at[4 + j], mate).wait_send()
    for b in range(2):
        remote(any_tiles(BLOCKS), sib.at[0], sib_send.at[b], sib_recv.at[0, 0], mate).wait_send()

    def drain(r):
        @pl.when(r >= ROUNDS - NACC)
        def _():
            for j in range(3):
                rs_wait(r, j)

        for j in range(3):
            part = wst.at[0, 0, top(TILES << j)]
            remote(part, part, ag_send.at[r, j], ag_recv.at[r, 0, j], mate).wait_send()
        for j in range(4):
            part = wst.at[0, 0, top(TILES << max(j - 1, 0))]
            remote(part, part, fw_send.at[r, j], fw_recv.at[r, j], mate).wait_send()
            remote(part, part, fw_send.at[r, j], fw_recv.at[r, j], mate).wait_recv()

    loop(ROUNDS, drain)
    wait_out(1, ROWS)
    wait_out(0, BROWS)


def comm_call(grads, gb, olds, mvwb):
    any_spec = pl.BlockSpec(memory_space=pl.ANY)
    vmem_spec = pl.BlockSpec(memory_space=pltpu.VMEM)
    f32, bf16 = jnp.float32, jnp.bfloat16
    dma = pltpu.SemaphoreType.DMA
    flat = jax.ShapeDtypeStruct((OUT_ROWS * LANES,), f32)
    return pl.pallas_call(
        comm_kernel,
        name='adam_comm',
        out_shape=(
            jax.ShapeDtypeStruct((2, ROUNDS, BLOCKS) + TILE, bf16), flat, flat, flat,
            jax.ShapeDtypeStruct((BROWS, LANES), bf16),
        ),
        in_specs=[any_spec] * 4 + [vmem_spec] + [any_spec] * 3 + [vmem_spec],
        out_specs=(any_spec,) * 4 + (vmem_spec,),
        scratch_shapes=[
            pltpu.VMEM((NACC, BLOCKS) + TILE, f32),
            pltpu.VMEM((2, BLOCKS) + TILE, f32),
            pltpu.VMEM((ROUNDS, BLOCKS // 2) + TILE, f32),
            pltpu.VMEM((ROUNDS, BLOCKS // 4) + TILE, f32),
            pltpu.VMEM((ROUNDS, TILES) + TILE, f32),
            pltpu.VMEM((2 * 3 * RAW_ROWS * LANES,), f32),
            pltpu.VMEM((3, RAW_ROWS, LANES), f32),
            pltpu.VMEM((3, ROWS + 8, LANES), f32),
            pltpu.VMEM((2 * 3 * ROWS * LANES,), f32),
            pltpu.VMEM((3, BROWS, LANES), f32),
            pltpu.VMEM((ROUNDS, TILES) + TILE, bf16),
            pltpu.VMEM((3, BROWS, LANES), f32),
            pltpu.VMEM((4, BROWS, LANES), f32),
            pltpu.VMEM((3, BROWS, LANES), f32),
            pltpu.VMEM((4, BROWS, LANES), bf16),
            pltpu.VMEM((4, BROWS, LANES), bf16),
            dma((NACC, 2)), dma((2,)), dma((2, 2)),
            dma((ROUNDS, 3)), dma((ROUNDS, 3, 3)),
            dma((ROUNDS, 3)), dma((ROUNDS, 3, 3)),
            dma((ROUNDS, 4)), dma((ROUNDS, 4)),
            dma((ROUNDS,)), dma((2,)), dma((2,)),
            dma((8,)), dma((8,)), dma((2,)), dma((2,)),
            pltpu.SemaphoreType.REGULAR,
        ],
        compiler_params=pltpu.CompilerParams(collective_id=0, has_side_effects=True, vmem_limit_bytes=67043328),
    )(*grads, gb, *olds, mvwb)


RING = 48
AHEAD = 28
CHIP_BLOCK = ROWS * LANES
CHIP_COUNT = 1968576
PARTS = 20
PER_PART = TENSOR_GROUPS[-1] // PARTS


def chip_group(pair, i):
    j = i - 2
    wide = 16 + 48 * (j // 6) + 24 * ((j % 6) // 3) + 3 * pair + j % 3
    first = jnp.where(i < 2, 1, 0)
    return first * (2 * pair + i) + (1 - first) * wide


def put_rows(rows, chip, first, count):
    def body(k):
        row = pl.multiple_of(first + k * 8, 8)
        flat = rows[pl.ds(row, 8), :].reshape(1, TILE_SIZE).astype(jnp.bfloat16)
        chip[:, pl.ds(pl.multiple_of(row * LANES, TILE_SIZE), TILE_SIZE)] = flat

    loop(count // 8, body, unroll=True)


def flatten_group(i, tiles, rows, chip, quarter):
    wide = (i >= 2) & (i < 14)

    def relay(stride):
        for u in range(4):
            row = quarter * 192 + u * (48 if stride == 6 else 6)
            for j in range(6):
                rows[pl.ds(row + j, 8, stride=stride), :] = tiles[quarter * 24 + u * 6 + j].astype(jnp.float32)

    @pl.when(wide)
    def _():
        relay(24)

    @pl.when(jnp.logical_not(wide))
    def _():
        relay(6)

    put_rows(rows, chip, quarter * 192, 192)


def unpack_kernel(wst, tail, we, wa, wf, wh, chip, buf, tiles, rows, where, in_sem, out_sem, sem):
    me = device_number()
    bits = chip_bits(me)
    pair = me // 2
    outs = (we, wa, wf, wh)
    total = TENSOR_GROUPS[-1]
    i = pl.program_id(0)

    def fill(d):
        diff = [(p + q) % 2 for p, q in zip(bits, chip_bits(d))]
        rels = [sum((1 << j) * diff[(k + j) % 3] for j in range(3)) for k in range(3)]
        for r in range(ROUNDS):
            for t, n, first, base in SLOTS:
                at = ((d % 2) * ROUNDS + r) * BLOCKS + base + rels[(t + r) % 3] * n
                where[(d * ROUNDS + r) * 3 + t] = at

    def fetch(group, dst, sem):
        for t, n, first, base in SLOTS:
            src = wst.at[pl.ds(where[group * 3 + t], n)]
            pltpu.make_async_copy(src, dst.at[pl.ds(first, n)], sem).start()

    def fetch_wait(dst, sem):
        pltpu.make_async_copy(wst.at[top(TILES)], dst, sem).wait()

    def start_in(g):
        slot = lax.rem(g, RING)
        fetch(g, buf.at[slot], in_sem.at[slot])

    def wait_out(g):
        slot = lax.rem(g, RING)
        pltpu.make_async_copy(buf.at[slot], wa.at[top(TILES)], out_sem.at[slot]).wait()

    def move(g):
        nxt = g + AHEAD

        @pl.when(nxt < total)
        def _():
            @pl.when(nxt >= RING)
            def _():
                wait_out(nxt)

            start_in(nxt)

        slot = lax.rem(g, RING)
        fetch_wait(buf.at[slot], in_sem.at[slot])
        for ref, lo, hi in zip(outs, TENSOR_GROUPS, TENSOR_GROUPS[1:]):
            @pl.when((g >= lo) & (g < hi))
            def _(ref=ref, lo=lo):
                pltpu.make_async_copy(buf.at[slot], ref.at[pl.ds((g - lo) * TILES, TILES)], out_sem.at[slot]).start()

    def start_part(k):
        fetch(chip_group(pair, k), tiles.at[k % 2], sem.at[k % 2])

    @pl.when(i == 0)
    def _():
        loop(2 * 8, fill)
        loop(AHEAD, start_in)
        start_part(0)

    @pl.when(i + 1 < PARTS)
    def _():
        start_part(i + 1)

    @pl.when(i < PARTS)
    def _():
        slot = i % 2
        fetch_wait(tiles.at[slot], sem.at[slot])

        def body(quarter):
            for k in range(2):
                move(i * PER_PART + quarter * 2 + k)
            flatten_group(i, tiles.at[slot], rows, chip, quarter)

        loop(PER_PART // 2, body)

    @pl.when(i == PARTS)
    def _():
        put_rows(tail, chip, 0, 24)
        loop(RING, wait_out)


def unpack_call(wst, tail):
    any_spec = pl.BlockSpec(memory_space=pl.ANY)
    sizes = [hi - lo for lo, hi in zip(TENSOR_GROUPS, TENSOR_GROUPS[1:])]
    bf16 = jnp.bfloat16
    dma = pltpu.SemaphoreType.DMA
    return pl.pallas_call(
        unpack_kernel,
        name='unpack',
        grid=(PARTS + 1,),
        out_shape=tuple(jax.ShapeDtypeStruct((n * TILES,) + TILE, bf16) for n in sizes)
        + (jax.ShapeDtypeStruct((1, CHIP_COUNT), bf16),),
        in_specs=[any_spec, pl.BlockSpec((24, LANES), lambda i: (0, 0))],
        out_specs=(any_spec,) * 4 + (pl.BlockSpec((1, CHIP_BLOCK), lambda i: (0, i)),),
        scratch_shapes=[
            pltpu.VMEM((RING, TILES) + TILE, bf16),
            pltpu.VMEM((2, TILES) + TILE, bf16),
            pltpu.VMEM((ROWS, LANES), jnp.float32),
            pltpu.SMEM((3 * TENSOR_GROUPS[-1],), jnp.int32),
            dma((RING,)), dma((RING,)), dma((2,)),
        ],
    )(wst, tail)


def to_tiles(x):
    width = x.shape[-1] // LANES
    return x.reshape(-1, 8, width, LANES).transpose(0, 2, 1, 3).reshape(-1, 8, LANES)


def from_tiles(x, shape):
    width = shape[-1] // LANES
    return x.reshape(-1, width, 8, LANES).transpose(0, 2, 1, 3).reshape(shape)


def solution(mesh):
    def local_step(g_embed, g_attn, g_ffn_in, g_ffn_out, g_vec, m_shard, v_shard, w_shard):
        d = device_number()
        mats = (g_embed, g_attn, g_ffn_in, g_ffn_out)
        shapes = [g.shape[1:] for g in mats]
        grads = [to_tiles(g) for g in mats]
        gb = jnp.pad(g_vec.reshape(-1, LANES), ((BPAD, 0), (0, 0)))
        shards = (m_shard, v_shard, w_shard)
        ends = jnp.stack([x[SHARD - BTAIL:].reshape(-1, LANES) for x in shards])
        mvwb = jnp.pad(ends, ((0, 0), (BPAD, 0), (0, 0)))
        wst, *new, wb = comm_call(grads, gb, shards, mvwb)
        new = [lax.slice(x, (BROWS * LANES,), (BROWS * LANES + SHARD,)) for x in new]
        wb_vec = wb[BPAD:].reshape(g_vec.shape[1:])
        part = g_vec.shape[2] // 8
        tail = lax.dynamic_slice(wb_vec, (0, (d // 2) * part), (2, part)).reshape(-1).astype(jnp.float32)
        tail = jnp.pad(tail, (0, 24 * LANES - 2 * part)).reshape(24, LANES)
        *packed, chip = unpack_call(wst.reshape((-1,) + TILE), tail)
        tensors = [from_tiles(x, shape) for x, shape in zip(packed, shapes)]
        return tuple(new) + tuple(tensors) + (wb_vec, chip)

    return jax.shard_map(local_step, mesh=mesh, in_specs=(P(MESH_AXES),) * 8,
                         out_specs=(P(MESH_AXES),) * 3 + (P(),) * 5 + (P(MESH_AXES),), check_vma=False)
```

```python
import jax
import jax.numpy as jnp
from jax import lax
from jax.experimental import pallas as pl
from jax.experimental.pallas import tpu as pltpu
from jax.sharding import PartitionSpec as P

MESH_AXES = ('outer', 'middle', 'inner')
ADAM_BETA1 = 0.9
ADAM_BETA2 = 0.98
ADAM_EPS = 1e-9
LEARN_RATE = 0.05
ADAM_STEP = 3

TILE = (8, 128)
LANES = TILE[1]
TILE_SIZE = 1024
ROUNDS = 10
TILES = 96
SLOTS = ((0, 36, 0, 0), (1, 30, 36, 288), (2, 30, 66, 528))
BLOCKS = 8 * TILES
TENSOR_GROUPS = (0, 16, 64, 112, 160)
ROWS = 768
FLAT = ROUNDS * ROWS * 128
SHARD = 984288
STEP = SHARD - FLAT
BTAIL = 16 * STEP
BROWS = 160
BPAD = BROWS - BTAIL // 128
RAW_ROWS = ROWS + BROWS
PARTS = 20
NEW_ROWS = ROUNDS * ROWS // PARTS
OUT_ROWS = NEW_ROWS + ROUNDS * ROWS + BROWS
NACC = 5
STAGES = ROUNDS + 6
MESH = pl.DeviceIdType.MESH


def loop(count, body, **options):
    lax.fori_loop(0, count, lambda i, carry: (body(i), carry)[1], None, **options)


def top(n):
    return pl.ds(0, n)


def device_number():
    return (lax.axis_index('outer') * 2 + lax.axis_index('middle')) * 4 + lax.axis_index('inner')


def mesh_id(d):
    return (d // 8, (d // 4) % 2, d % 4)


def adam_update(grad_mean, m_old, v_old, w_old):
    m_new = ADAM_BETA1 * m_old + (1.0 - ADAM_BETA1) * grad_mean
    v_new = ADAM_BETA2 * v_old + (1.0 - ADAM_BETA2) * (grad_mean * grad_mean)
    m_hat = m_new / (1.0 - ADAM_BETA1 ** ADAM_STEP)
    v_hat = v_new / (1.0 - ADAM_BETA2 ** ADAM_STEP)
    w_new = w_old - LEARN_RATE * m_hat / (jnp.sqrt(v_hat) + ADAM_EPS)
    return m_new, v_new, w_new


def axis_weights(a):
    return ((a - 1) * (a - 2)) // 2, a * (2 - a), (a * (a - 1)) // 2


def pick(values, a):
    e0, e1, e2 = axis_weights(a)
    return values[0] * e0 + values[1] * e1 + values[2] * e2


def chip_bits(d):
    return (d // 2) % 2, (d // 4) % 2, d // 8


def comm_kernel(ge, ga, gf, gh, gvec, m1, v1, w1, ends,
                wst, m_out, v_out, w_out, wb_out,
                acc, sib, l1, l2, l3, flat_in, raw, mv, flat_out, heads, wt, mvwb, gb, bs, bl, bout, wbs, wbl,
                own_sem, sib_send, sib_recv, rs_send, rs_recv, ag_send, ag_recv, fw_send, fw_recv,
                loc_sem, in_sem, out_sem, b_send, b_recv, end_sem, head_sem, free_sem):
    me = device_number()
    core = me % 2
    mate = me + 1 - 2 * core
    bits = chip_bits(me)
    deltas = tuple(m * (1 - 2 * b) for m, b in zip((2, 4, 8), bits))
    partners = (mate,) + tuple(me + d for d in deltas)
    grads = (ge, ga, gf, gh)
    olds = tuple(enumerate((m1, v1, w1)))
    outs = tuple(enumerate((m_out, v_out, w_out)))
    shift_rows = (STEP * me) // LANES
    shift_lanes = (STEP * me) % LANES
    back_lanes = (LANES - shift_lanes) % LANES
    lane = lax.broadcasted_iota(jnp.int32, TILE, 1)

    barrier = pltpu.get_barrier_semaphore()
    for other in partners + ((me + 1) % 16, (me + 15) % 16):
        pl.semaphore_signal(barrier, inc=1, device_id=mesh_id(other), device_id_type=MESH)
    pl.semaphore_wait(barrier, 6)

    def remote(src, dst, ssem, rsem, dev):
        return pltpu.make_async_remote_copy(src_ref=src, dst_ref=dst, send_sem=ssem, recv_sem=rsem,
                                            device_id=mesh_id(dev), device_id_type=MESH)

    def turned(r):
        steps = [pick(deltas, lax.rem(2 * r + j, 3)) for j in range(3)]
        return [[steps[(t + j) % 3] for j in range(3)] for t in range(3)]

    def block(d, r, first, n):
        return wst.at[pl.ds((d * ROUNDS + r) * TILES + first, n)]

    def any_tiles(n):
        return ga.at[top(n)]

    def rs_wait(r, j):
        half = acc.at[0, top(BLOCKS // 2 >> j)]
        remote(half, half, rs_send.at[r, j], rs_recv.at[r, 0, j], mate).wait_send()

    def load_round(r):
        a = r % NACC
        b = r % 2

        steps = turned(r)

        def body(back):
            rel = 7 - back
            betas = (rel // 4, (rel // 2) % 2, rel % 2)
            for t, n, first, base in SLOTS:
                d = me + sum(beta * step for beta, step in zip(betas, steps[t]))
                at = pl.ds(base + rel * n, n)
                for other in (False, True):
                    group = ROUNDS * (d + (mate - me if other else 0)) + r
                    for ref, lo, hi in zip(grads, TENSOR_GROUPS, TENSOR_GROUPS[1:]):
                        @pl.when((group >= lo) & (group < hi))
                        def _(ref=ref, lo=lo, other=other, group=group):
                            src = ref.at[pl.ds((group - lo) * TILES + first, n)]
                            if other:
                                remote(src, sib.at[b, at], sib_send.at[b], sib_recv.at[b, rel // 4], mate).start()
                            else:
                                pltpu.make_async_copy(src, acc.at[a, at], own_sem.at[a, rel // 4]).start()

        loop(8, body)

    def add_range(dst, src, n):
        def body(i):
            at = pl.ds(i * 6, 6)
            dst[at] = dst[at] + src[at]

        loop(n // 6, body)

    def when_round(r):
        return pl.when((r >= 0) & (r < ROUNDS))

    def old_copy(ref, r, i, skip):
        n = (RAW_ROWS - skip) * LANES
        at = ((r % 2 * 3 + i) * RAW_ROWS + skip) * LANES
        return pltpu.make_async_copy(ref.at[pl.ds((r * ROWS - BROWS + skip) * LANES, n)], flat_in.at[pl.ds(at, n)],
                                     in_sem.at[r % 2])

    def old_rows(r, skip):
        for i, ref in olds:
            old_copy(ref, r, i, skip).wait()

        def body(k):
            row = skip + k * 8
            for i, ref in olds:
                at = ((r % 2 * 3 + i) * RAW_ROWS + row) * LANES
                raw[i, pl.ds(row, 8), :] = flat_in[pl.ds(pl.multiple_of(at, TILE_SIZE), TILE_SIZE)].reshape(TILE)

        loop((RAW_ROWS - skip) // 8, body)

    def out_copy(ref, b, i, r, n):
        at = pl.multiple_of((r * ROWS + NEW_ROWS - 1 - shift_rows) * LANES, LANES)
        return pltpu.make_async_copy(flat_out.at[pl.ds((b * 3 + i) * ROWS * LANES, n * LANES)], ref.at[pl.ds(at, n * LANES)],
                                     out_sem.at[b])

    def put_out(b, r, n):
        def body(k):
            for i, ref in outs:
                low = pltpu.roll(mv[i, pl.ds(k * 8 + 7, 8), :], back_lanes, 1)
                high = pltpu.roll(mv[i, pl.ds(k * 8 + 8, 8), :], back_lanes, 1)
                at = ((b * 3 + i) * ROWS + k * 8) * LANES
                both = jnp.where(lane < LANES - shift_lanes, low, high)
                flat_out[pl.ds(pl.multiple_of(at, TILE_SIZE), TILE_SIZE)] = both.reshape(TILE_SIZE)

        loop(n // 8, body)
        for i, ref in outs:
            out_copy(ref, b, i, r, n).start()

    def wait_out(b, n):
        for i, ref in outs:
            out_copy(ref, b, i, 0, n).wait()

    load_round(0)

    gb[...] = jnp.zeros_like(gb)
    mvwb[...] = jnp.zeros_like(mvwb)
    for i, ref in olds:
        mvwb[i, pl.ds(BPAD, BROWS - BPAD), :] = ends[pl.ds(i * (BROWS - BPAD), BROWS - BPAD), :]
    for i in range(2):
        def spread(k, i=i):
            row = BPAD + i * (BTAIL // LANES // 2) + k
            gb[pl.ds(row, 1), :] = gvec[pl.ds(i, 1), pl.ds(pl.multiple_of(k * LANES, LANES), LANES)]

        loop(BTAIL // LANES // 2, spread)

    @pl.when(me < 15)
    def _():
        remote(mvwb, raw.at[:, top(BROWS)], end_sem.at[0], end_sem.at[1], me + 1).start()

    def stage(s):
        nxt = s + 1

        @pl.when((nxt >= NACC) & (nxt < ROUNDS))
        def _():
            for j in range(3):
                rs_wait(nxt - NACC, j)

        @pl.when((nxt >= 2) & (nxt < ROUNDS))
        def _():
            remote(any_tiles(BLOCKS), sib.at[0], sib_send.at[nxt % 2], sib_recv.at[0, 0], mate).wait_send()
            pl.semaphore_wait(free_sem, 1)

        @pl.when(nxt < ROUNDS)
        def _():
            load_round(nxt)

        @pl.when(s == 2)
        def _():
            for i, ref in olds:
                old_copy(ref, 0, i, BROWS).start()

        @pl.when((s > 2) & (s < ROUNDS + 2))
        def _():
            for i, ref in olds:
                old_copy(ref, s - 2, i, 0).start()

        @when_round(s)
        def _():
            r, a, b = s, s % NACC, s % 2
            steps = turned(r)

            def loaded(part):
                src, half = any_tiles(BLOCKS // 2), top(BLOCKS // 2)
                pltpu.make_async_copy(src, acc.at[a, half], own_sem.at[a, part]).wait()
                remote(src, sib.at[b, half], sib_send.at[b], sib_recv.at[b, part], mate).wait_recv()

            loaded(1)
            for t, n, first, base in SLOTS:
                hi = pl.ds(base + 4 * n, 4 * n)
                add_range(acc.at[a, hi], sib.at[b, hi], 4 * n)
            for t, n, first, base in SLOTS:
                remote(acc.at[a, pl.ds(base + 4 * n, 4 * n)], l1.at[r, pl.ds(base // 2, 4 * n)],
                       rs_send.at[r, 0], rs_recv.at[r, t, 0], me + steps[t][0]).start()
            loaded(0)
            for t, n, first, base in SLOTS:
                lo = pl.ds(base, 4 * n)
                add_range(acc.at[a, lo], sib.at[b, lo], 4 * n)

            @pl.when(r + 2 < ROUNDS)
            def _():
                pl.semaphore_signal(free_sem, inc=1, device_id=mesh_id(mate), device_id_type=MESH)

        for j, land, out in ((1, l1, l2), (2, l2, l3)):
            @when_round(s - j)
            def _(j=j, land=land, out=out):
                r = s - j
                a = r % NACC
                keep = 4 >> j
                steps = turned(r)
                for t, n, first, base in SLOTS:
                    here = land.at[r, pl.ds(base >> j, 2 * keep * n)]
                    remote(here, here, rs_send.at[r, j - 1], rs_recv.at[r, t, j - 1], mate).wait_recv()
                    add_range(acc.at[a, pl.ds(base + keep * n, keep * n)],
                              land.at[r, pl.ds((base >> j) + keep * n, keep * n)], keep * n)
                for t, n, first, base in SLOTS:
                    remote(acc.at[a, pl.ds(base + keep * n, keep * n)], out.at[r, pl.ds(base >> (j + 1), keep * n)],
                           rs_send.at[r, j], rs_recv.at[r, t, j], me + steps[t][j]).start()
                for t, n, first, base in SLOTS:
                    add_range(acc.at[a, pl.ds(base, keep * n)], land.at[r, pl.ds(base >> j, keep * n)], keep * n)

        @when_round(s - 3)
        def _():
            r = s - 3
            a, b = r % NACC, r % 2

            @pl.when(r == 0)
            def _():
                old_rows(0, BROWS)

            @pl.when((r == 0) & (me > 0))
            def _():
                remote(mvwb, raw.at[:, top(BROWS)], end_sem.at[0], end_sem.at[1], mate).wait_recv()

            @pl.when(r > 0)
            def _():
                old_rows(r, 0)

            @pl.when((r == 1) & (me > 0))
            def _():
                remote(mv.at[:, pl.ds(8, BROWS)], heads, head_sem.at[0], head_sem.at[1], mate).wait_send()

            for i, ref in outs:
                mv[i, pl.ds(7, 1), :] = mv[i, pl.ds(ROWS + 7, 1), :]
            for t, n, first, base in SLOTS:
                here = l3.at[r, pl.ds(first, n)]
                remote(here, here, rs_send.at[r, 2], rs_recv.at[r, t, 2], mate).wait_recv()
            steps = turned(r)
            group = ROUNDS * me + r
            wide = (group >= TENSOR_GROUPS[1]) & (group < TENSOR_GROUPS[3])

            def adam_pass(stride):
                for t, n, first, base in SLOTS:
                    def body(u, first=first, base=base):
                        unit = first // 6 + u
                        if stride == 6:
                            row = unit * 48
                        else:
                            row = (unit // 4) * 192 + (unit % 4) * 6
                        for j in range(6):
                            old = []
                            for i, ref in olds:
                                at = row + j + BROWS - shift_rows
                                here = pltpu.roll(raw[i, pl.ds(at, 8, stride=stride), :], shift_lanes, 1)
                                prev = pltpu.roll(raw[i, pl.ds(at - 1, 8, stride=stride), :], shift_lanes, 1)
                                old.append(jnp.where(lane >= shift_lanes, here, prev))
                            tile = acc[a, base + u * 6 + j] + l3[r, unit * 6 + j]
                            new = adam_update(tile * (1.0 / 16.0), *old)
                            for i, ref in olds:
                                mv[i, pl.ds(row + j + 8, 8, stride=stride), :] = new[i]
                            wt[r, unit * 6 + j] = new[2].astype(jnp.bfloat16)

                    loop(n // 6, body)

            @pl.when(wide)
            def _():
                adam_pass(24)

            @pl.when(jnp.logical_not(wide))
            def _():
                adam_pass(6)

            for t, n, first, base in SLOTS:
                remote(wt.at[r, pl.ds(first, n)], block(me, r, first, n), ag_send.at[r, 0], ag_recv.at[r, t, 0],
                       me + steps[t][0]).start()
            mine = block(me, r, 0, TILES)
            remote(wt.at[r], mine, fw_send.at[r, 0], fw_recv.at[r, 0], mate).start()
            pltpu.make_async_copy(wt.at[r], mine, loc_sem.at[r]).start()

            @pl.when((r == 0) & (me > 0))
            def _():
                remote(mv.at[:, pl.ds(8, BROWS)], heads, head_sem.at[0], head_sem.at[1], me - 1).start()

            @pl.when(r >= 2)
            def _():
                wait_out(b, ROWS)

            put_out(b, r, ROWS)

        @pl.when((s == ROUNDS + 3) & (me < 15))
        def _():
            remote(mvwb, raw.at[:, top(BROWS)], end_sem.at[0], end_sem.at[1], mate).wait_send()
            remote(mv.at[:, pl.ds(8, BROWS)], heads, head_sem.at[0], head_sem.at[1], mate).wait_recv()

        @pl.when(s == ROUNDS + 3)
        def _():
            wait_out(0, ROWS)
            for i, ref in outs:
                mv[i, pl.ds(7, 1), :] = mv[i, pl.ds(ROWS + 7, 1), :]
                mv[i, pl.ds(8, BROWS), :] = heads[i]
            put_out(0, ROUNDS, BROWS)

        for j in (1, 2, 3):
            @when_round(s - 3 - j)
            def _(j=j):
                r = s - 3 - j
                got = 1 << (j - 1)
                steps = turned(r)
                if j == 1:
                    pltpu.make_async_copy(wt.at[r], block(me, r, 0, TILES), loc_sem.at[r]).wait()
                for t, n, first, base in SLOTS:
                    part = wst.at[top(got * n)]
                    remote(part, part, ag_send.at[r, j - 1], ag_recv.at[r, t, j - 1], mate).wait_recv()
                    held = [me]
                    for step in steps[t][:j]:
                        held = held + [d + step for d in held]
                    if j < 3:
                        for d in held:
                            here = block(d, r, first, n)
                            remote(here, here, ag_send.at[r, j], ag_recv.at[r, t, j], me + steps[t][j]).start()
                    for d in held[got:]:
                        here = block(d, r, first, n)
                        remote(here, here, fw_send.at[r, j], fw_recv.at[r, j], mate).start()

        for j in range(9):
            @pl.when(s == j)
            def _(j=j):
                if j > 0:
                    i = j - 1
                    land = bl.at[i] if i < 4 else wbl.at[i - 4]
                    remote(land, land, b_send.at[i], b_recv.at[i], mate).wait_recv()
                if j < 4:
                    src = gb
                    if j > 0:
                        src = bs.at[j - 1]
                        src[...] = (gb[...] if j == 1 else bs[j - 2]) + bl[j - 1]
                    remote(src, bl.at[j], b_send.at[j], b_recv.at[j], partners[j]).start()
                elif j < 8:
                    if j == 4:
                        new = adam_update((bs[2] + bl[3]) * (1.0 / 16.0), mvwb[0], mvwb[1], mvwb[2])
                        for i, ref in outs:
                            bout[i] = new[i]
                        keep = jnp.broadcast_to(me, (BROWS, LANES)) == 15
                        wbs[0] = jnp.where(keep, new[2], 0.0).astype(jnp.bfloat16)

                        @pl.when(me == 15)
                        def _():
                            for i, ref in outs:
                                heads[i, top(BROWS - BPAD), :] = bout[i, pl.ds(BPAD, BROWS - BPAD), :]
                    else:
                        wbs[j - 4] = wbs[j - 5] + wbl[j - 5]
                    remote(wbs.at[j - 4], wbl.at[j - 4], b_send.at[j], b_recv.at[j], partners[j - 4]).start()
                else:
                    wb_out[...] = wbs[3] + wbl[3]

    loop(STAGES, stage)

    for j in range(4):
        remote(gb, bl.at[j], b_send.at[j], b_recv.at[j], mate).wait_send()
        remote(wbs.at[j], wbl.at[j], b_send.at[4 + j], b_recv.at[4 + j], mate).wait_send()
    for b in range(2):
        remote(any_tiles(BLOCKS), sib.at[0], sib_send.at[b], sib_recv.at[0, 0], mate).wait_send()

    def drain(r):
        @pl.when(r >= ROUNDS - NACC)
        def _():
            for j in range(3):
                rs_wait(r, j)

        for j in range(3):
            part = wst.at[top(TILES << j)]
            remote(part, part, ag_send.at[r, j], ag_recv.at[r, 0, j], mate).wait_send()
        for j in range(4):
            part = wst.at[top(TILES << max(j - 1, 0))]
            remote(part, part, fw_send.at[r, j], fw_recv.at[r, j], mate).wait_send()
            remote(part, part, fw_send.at[r, j], fw_recv.at[r, j], mate).wait_recv()

    loop(ROUNDS, drain)
    wait_out(1, ROWS)
    wait_out(0, BROWS)


def comm_call(grads, gvec, olds, ends):
    any_spec = pl.BlockSpec(memory_space=pl.ANY)
    vmem_spec = pl.BlockSpec(memory_space=pltpu.VMEM)
    f32, bf16 = jnp.float32, jnp.bfloat16
    dma = pltpu.SemaphoreType.DMA
    flat = jax.ShapeDtypeStruct((OUT_ROWS * LANES,), f32)
    return pl.pallas_call(
        comm_kernel,
        name='adam_comm',
        out_shape=(
            jax.ShapeDtypeStruct((TENSOR_GROUPS[-1] * TILES,) + TILE, bf16), flat, flat, flat,
            jax.ShapeDtypeStruct((BROWS, LANES), bf16),
        ),
        in_specs=[any_spec] * 4 + [vmem_spec] + [any_spec] * 3 + [vmem_spec],
        out_specs=(any_spec,) * 4 + (vmem_spec,),
        scratch_shapes=[
            pltpu.VMEM((NACC, BLOCKS) + TILE, f32),
            pltpu.VMEM((2, BLOCKS) + TILE, f32),
            pltpu.VMEM((ROUNDS, BLOCKS // 2) + TILE, f32),
            pltpu.VMEM((ROUNDS, BLOCKS // 4) + TILE, f32),
            pltpu.VMEM((ROUNDS, TILES) + TILE, f32),
            pltpu.VMEM((2 * 3 * RAW_ROWS * LANES,), f32),
            pltpu.VMEM((3, RAW_ROWS, LANES), f32),
            pltpu.VMEM((3, ROWS + 8, LANES), f32),
            pltpu.VMEM((2 * 3 * ROWS * LANES,), f32),
            pltpu.VMEM((3, BROWS, LANES), f32),
            pltpu.VMEM((ROUNDS, TILES) + TILE, bf16),
            pltpu.VMEM((3, BROWS, LANES), f32),
            pltpu.VMEM((BROWS, LANES), f32),
            pltpu.VMEM((3, BROWS, LANES), f32),
            pltpu.VMEM((4, BROWS, LANES), f32),
            pltpu.VMEM((3, BROWS, LANES), f32),
            pltpu.VMEM((4, BROWS, LANES), bf16),
            pltpu.VMEM((4, BROWS, LANES), bf16),
            dma((NACC, 2)), dma((2,)), dma((2, 2)),
            dma((ROUNDS, 3)), dma((ROUNDS, 3, 3)),
            dma((ROUNDS, 3)), dma((ROUNDS, 3, 3)),
            dma((ROUNDS, 4)), dma((ROUNDS, 4)),
            dma((ROUNDS,)), dma((2,)), dma((2,)),
            dma((8,)), dma((8,)), dma((2,)), dma((2,)),
            pltpu.SemaphoreType.REGULAR,
        ],
        compiler_params=pltpu.CompilerParams(collective_id=0, has_side_effects=True, vmem_limit_bytes=67043328),
    )(*grads, gvec, *olds, ends)


RING = 16
AHEAD = 8
HALF = BLOCKS // 2
MOVES = TENSOR_GROUPS[-1] * TILES // HALF
CHIP_BLOCK = ROWS * LANES
CHIP_COUNT = 1968576
PER_PART = TENSOR_GROUPS[-1] // PARTS


def chip_group(pair, i):
    j = i - 2
    wide = 16 + 48 * (j // 6) + 24 * ((j % 6) // 3) + 3 * pair + j % 3
    first = jnp.where(i < 2, 1, 0)
    return first * (2 * pair + i) + (1 - first) * wide


def put_rows(rows, chip, first, count):
    def body(k):
        row = pl.multiple_of(first + k * 8, 8)
        flat = rows[pl.ds(row, 8), :].reshape(1, TILE_SIZE).astype(jnp.bfloat16)
        chip[:, pl.ds(pl.multiple_of(row * LANES, TILE_SIZE), TILE_SIZE)] = flat

    loop(count // 8, body, unroll=True)


def flatten_group(i, tiles, rows, chip, quarter):
    wide = (i >= 2) & (i < 14)

    def relay(stride):
        for u in range(4):
            row = quarter * 192 + u * (48 if stride == 6 else 6)
            for j in range(6):
                rows[pl.ds(row + j, 8, stride=stride), :] = tiles[quarter * 24 + u * 6 + j].astype(jnp.float32)

    @pl.when(wide)
    def _():
        relay(24)

    @pl.when(jnp.logical_not(wide))
    def _():
        relay(6)

    put_rows(rows, chip, quarter * 192, 192)


def unpack_kernel(wst, tail, m1, v1, w1, we, wa, wf, wh, chip, m2, v2, w2, buf, tiles, rows,
                  in_sem, out_sem, sem):
    me = device_number()
    pair = me // 2
    outs = (we, wa, wf, wh)
    i = pl.program_id(0)
    news = ((m1, m2), (v1, v2), (w1, w2))

    def some(k):
        return wst.at[pl.ds(k * HALF, HALF)]

    def start_in(k):
        slot = lax.rem(k, RING)
        pltpu.make_async_copy(some(k), buf.at[slot], in_sem.at[slot]).start()

    def wait_out(k):
        slot = lax.rem(k, RING)
        pltpu.make_async_copy(buf.at[slot], wa.at[top(HALF)], out_sem.at[slot]).wait()

    def part_copy(k):
        src = wst.at[pl.ds(chip_group(pair, k) * TILES, TILES)]
        return pltpu.make_async_copy(src, tiles.at[k % 2], sem.at[k % 2])

    for src, dst in news:
        dst[...] = src[...]

    @pl.when(i == 0)
    def _():
        part_copy(0).start()
        loop(AHEAD, start_in)

    def move(k):
        nxt = k + AHEAD

        @pl.when((nxt >= RING) & (nxt < MOVES))
        def _():
            wait_out(nxt)

        @pl.when(nxt < MOVES)
        def _():
            start_in(nxt)

        slot = lax.rem(k, RING)
        pltpu.make_async_copy(some(k), buf.at[slot], in_sem.at[slot]).wait()
        for ref, lo, hi in zip(outs, TENSOR_GROUPS, TENSOR_GROUPS[1:]):
            @pl.when((i * PER_PART >= lo) & (i * PER_PART < hi))
            def _(ref=ref, lo=lo):
                dst = ref.at[pl.ds(k * HALF - lo * TILES, HALF)]
                pltpu.make_async_copy(buf.at[slot], dst, out_sem.at[slot]).start()

    @pl.when(i + 1 < PARTS)
    def _():
        part_copy(i + 1).start()

    @pl.when(i < PARTS)
    def _():
        part_copy(i).wait()
        for k in range(2):
            move(2 * i + k)
            loop(2, lambda q: flatten_group(i, tiles.at[i % 2], rows, chip, 2 * k + q))

    @pl.when(i == PARTS)
    def _():
        put_rows(tail, chip, 0, 24)
        loop(RING, wait_out)


def unpack_call(wst, tail, new):
    any_spec = pl.BlockSpec(memory_space=pl.ANY)
    sizes = [hi - lo for lo, hi in zip(TENSOR_GROUPS, TENSOR_GROUPS[1:])]
    bf16 = jnp.bfloat16
    dma = pltpu.SemaphoreType.DMA
    return pl.pallas_call(
        unpack_kernel,
        name='unpack',
        grid=(PARTS + 1,),
        out_shape=tuple(jax.ShapeDtypeStruct((n * TILES,) + TILE, bf16) for n in sizes)
        + (jax.ShapeDtypeStruct((1, CHIP_COUNT), bf16),) + (jax.ShapeDtypeStruct((SHARD,), jnp.float32),) * 3,
        in_specs=[any_spec, pl.BlockSpec((24, LANES), lambda i: (0, 0))] + [pl.BlockSpec((NEW_ROWS * LANES,), lambda i: (i + 1,))] * 3,
        out_specs=(any_spec,) * 4 + (pl.BlockSpec((1, CHIP_BLOCK), lambda i: (0, i)),)
        + (pl.BlockSpec((NEW_ROWS * LANES,), lambda i: (i,)),) * 3,
        scratch_shapes=[
            pltpu.VMEM((RING, HALF) + TILE, bf16),
            pltpu.VMEM((2, TILES) + TILE, bf16),
            pltpu.VMEM((ROWS, LANES), jnp.float32),
            dma((RING,)), dma((RING,)), dma((2,)),
        ],
    )(wst, tail, *new)


def to_tiles(x):
    width = x.shape[-1] // LANES
    return x.reshape(-1, 8, width, LANES).transpose(0, 2, 1, 3).reshape(-1, 8, LANES)


def from_tiles(x, shape):
    width = shape[-1] // LANES
    return x.reshape(-1, width, 8, LANES).transpose(0, 2, 1, 3).reshape(shape)


def solution(mesh):
    def local_step(g_embed, g_attn, g_ffn_in, g_ffn_out, g_vec, m_shard, v_shard, w_shard):
        d = device_number()
        mats = (g_embed, g_attn, g_ffn_in, g_ffn_out)
        shapes = [g.shape[1:] for g in mats]
        grads = [to_tiles(g) for g in mats]
        shards = (m_shard, v_shard, w_shard)
        ends = jnp.concatenate([x[SHARD - BTAIL:] for x in shards]).reshape(-1, LANES)
        wst, *new, wb = comm_call(grads, g_vec[0], shards, ends)
        wb_vec = wb[BPAD:].reshape(g_vec.shape[1:])
        part = g_vec.shape[2] // 8
        tail = lax.dynamic_slice(wb_vec, (0, (d // 2) * part), (2, part)).reshape(-1).astype(jnp.float32)
        tail = jnp.pad(tail, (0, 24 * LANES - 2 * part)).reshape(24, LANES)
        *packed, chip, m_new, v_new, w_new = unpack_call(wst, tail, new)
        tensors = [from_tiles(x, shape) for x, shape in zip(packed, shapes)]
        return (m_new, v_new, w_new) + tuple(tensors) + (wb_vec, chip)

    return jax.shard_map(local_step, mesh=mesh, in_specs=(P(MESH_AXES),) * 8,
                         out_specs=(P(MESH_AXES),) * 3 + (P(),) * 5 + (P(MESH_AXES),), check_vma=False)
```

```python
import jax
import jax.numpy as jnp
from jax import lax
from jax.experimental import pallas as pl
from jax.experimental.pallas import tpu as pltpu
from jax.sharding import PartitionSpec as P

MESH_AXES = ('outer', 'middle', 'inner')
ADAM_BETA1 = 0.9
ADAM_BETA2 = 0.98
ADAM_EPS = 1e-9
LEARN_RATE = 0.05
ADAM_STEP = 3

TILE = (8, 128)
LANES = TILE[1]
TILE_SIZE = 1024
ROUNDS = 10
TILES = 96
SLOTS = ((0, 36, 0, 0), (1, 30, 36, 288), (2, 30, 66, 528))
BLOCKS = 8 * TILES
TENSOR_GROUPS = (0, 16, 64, 112, 160)
ROWS = 768
FLAT = ROUNDS * ROWS * 128
SHARD = 984288
STEP = SHARD - FLAT
BTAIL = 16 * STEP
BROWS = 160
BPAD = BROWS - BTAIL // 128
RAW_ROWS = ROWS + BROWS
PARTS = 20
NEW_ROWS = ROUNDS * ROWS // PARTS
OUT_ROWS = NEW_ROWS + ROUNDS * ROWS + BROWS
NACC = 5
STAGES = ROUNDS + 6
MESH = pl.DeviceIdType.MESH


def loop(count, body, **options):
    lax.fori_loop(0, count, lambda i, carry: (body(i), carry)[1], None, **options)


def top(n):
    return pl.ds(0, n)


def device_number():
    return (lax.axis_index('outer') * 2 + lax.axis_index('middle')) * 4 + lax.axis_index('inner')


def mesh_id(d):
    return (d // 8, (d // 4) % 2, d % 4)


def adam_update(grad_mean, m_old, v_old, w_old):
    m_new = ADAM_BETA1 * m_old + (1.0 - ADAM_BETA1) * grad_mean
    v_new = ADAM_BETA2 * v_old + (1.0 - ADAM_BETA2) * (grad_mean * grad_mean)
    m_hat = m_new / (1.0 - ADAM_BETA1 ** ADAM_STEP)
    v_hat = v_new / (1.0 - ADAM_BETA2 ** ADAM_STEP)
    w_new = w_old - LEARN_RATE * m_hat / (jnp.sqrt(v_hat) + ADAM_EPS)
    return m_new, v_new, w_new


def axis_weights(a):
    return ((a - 1) * (a - 2)) // 2, a * (2 - a), (a * (a - 1)) // 2


def pick(values, a):
    e0, e1, e2 = axis_weights(a)
    return values[0] * e0 + values[1] * e1 + values[2] * e2


def chip_bits(d):
    return (d // 2) % 2, (d // 4) % 2, d // 8


def comm_kernel(ge, ga, gf, gh, gvec, m1, v1, w1, ends,
                wst, m_out, v_out, w_out, wb_out,
                acc, sib, l1, l2, l3, flat_in, raw, mv, flat_out, heads, wt, mvwb, gb, bs, bl, bout, wbs, wbl,
                own_sem, sib_send, sib_recv, rs_send, rs_recv, ag_send, ag_recv, fw_send, fw_recv,
                loc_sem, in_sem, out_sem, b_send, b_recv, end_sem, head_sem, free_sem):
    me = device_number()
    core = me % 2
    mate = me + 1 - 2 * core
    bits = chip_bits(me)
    deltas = tuple(m * (1 - 2 * b) for m, b in zip((2, 4, 8), bits))
    partners = (mate,) + tuple(me + d for d in deltas)
    grads = (ge, ga, gf, gh)
    olds = tuple(enumerate((m1, v1, w1)))
    outs = tuple(enumerate((m_out, v_out, w_out)))
    shift_rows = (STEP * me) // LANES
    shift_lanes = (STEP * me) % LANES
    back_lanes = (LANES - shift_lanes) % LANES
    lane = lax.broadcasted_iota(jnp.int32, TILE, 1)

    barrier = pltpu.get_barrier_semaphore()
    for other in partners + ((me + 1) % 16, (me + 15) % 16):
        pl.semaphore_signal(barrier, inc=1, device_id=mesh_id(other), device_id_type=MESH)
    pl.semaphore_wait(barrier, 6)

    def remote(src, dst, ssem, rsem, dev):
        return pltpu.make_async_remote_copy(src_ref=src, dst_ref=dst, send_sem=ssem, recv_sem=rsem,
                                            device_id=mesh_id(dev), device_id_type=MESH)

    def sized(number, use):
        for c in range(4):
            @pl.when((number + 3) // 4 == c + 1)
            def _(c=c):
                use((c + 1) * BROWS // 4)

    def ends_copy(n, dev):
        at = pl.ds(BROWS - n, n)
        return remote(mvwb.at[:, at], raw.at[:, at], end_sem.at[0], end_sem.at[1], dev)

    def heads_copy(n, dev):
        return remote(mv.at[:, pl.ds(8, n)], heads.at[:, top(n)], head_sem.at[0], head_sem.at[1], dev)

    def turned(r):
        steps = [pick(deltas, lax.rem(2 * r + j, 3)) for j in range(3)]
        return [[steps[(t + j) % 3] for j in range(3)] for t in range(3)]

    def block(d, r, first, n):
        return wst.at[pl.ds((d * ROUNDS + r) * TILES + first, n)]

    def any_tiles(n):
        return ga.at[top(n)]

    def rs_wait(r, j):
        half = acc.at[0, top(BLOCKS // 2 >> j)]
        remote(half, half, rs_send.at[r, j], rs_recv.at[r, 0, j], mate).wait_send()

    def load_round(r):
        a = r % NACC
        b = r % 2

        steps = turned(r)

        def body(back):
            rel = 7 - back
            betas = (rel // 4, (rel // 2) % 2, rel % 2)
            for t, n, first, base in SLOTS:
                d = me + sum(beta * step for beta, step in zip(betas, steps[t]))
                at = pl.ds(base + rel * n, n)
                for other in (False, True):
                    group = ROUNDS * (d + (mate - me if other else 0)) + r
                    for ref, lo, hi in zip(grads, TENSOR_GROUPS, TENSOR_GROUPS[1:]):
                        @pl.when((group >= lo) & (group < hi))
                        def _(ref=ref, lo=lo, other=other, group=group):
                            src = ref.at[pl.ds((group - lo) * TILES + first, n)]
                            if other:
                                remote(src, sib.at[b, at], sib_send.at[b], sib_recv.at[b, rel], mate).start()
                            else:
                                pltpu.make_async_copy(src, acc.at[a, at], own_sem.at[a, rel]).start()

        loop(8, body)

    def add_range(dst, src, n):
        def body(i):
            at = pl.ds(i * 6, 6)
            dst[at] = dst[at] + src[at]

        loop(n // 6, body)

    def when_round(r):
        return pl.when((r >= 0) & (r < ROUNDS))

    def old_copy(ref, r, i, skip):
        n = (RAW_ROWS - skip) * LANES
        at = ((r % 2 * 3 + i) * RAW_ROWS + skip) * LANES
        return pltpu.make_async_copy(ref.at[pl.ds((r * ROWS - BROWS + skip) * LANES, n)], flat_in.at[pl.ds(at, n)],
                                     in_sem.at[r % 2])

    def old_rows(r, skip):
        for i, ref in olds:
            old_copy(ref, r, i, skip).wait()

        def body(k):
            row = skip + k * 8
            for i, ref in olds:
                at = ((r % 2 * 3 + i) * RAW_ROWS + row) * LANES
                raw[i, pl.ds(row, 8), :] = flat_in[pl.ds(pl.multiple_of(at, TILE_SIZE), TILE_SIZE)].reshape(TILE)

        loop((RAW_ROWS - skip) // 8, body)

    def out_copy(ref, b, i, r, n):
        at = pl.multiple_of((r * ROWS + NEW_ROWS - 1 - shift_rows) * LANES, LANES)
        return pltpu.make_async_copy(flat_out.at[pl.ds((b * 3 + i) * ROWS * LANES, n * LANES)], ref.at[pl.ds(at, n * LANES)],
                                     out_sem.at[b])

    def put_out(b, r, n):
        def body(k):
            for i, ref in outs:
                low = pltpu.roll(mv[i, pl.ds(k * 8 + 7, 8), :], back_lanes, 1)
                high = pltpu.roll(mv[i, pl.ds(k * 8 + 8, 8), :], back_lanes, 1)
                at = ((b * 3 + i) * ROWS + k * 8) * LANES
                both = jnp.where(lane < LANES - shift_lanes, low, high)
                flat_out[pl.ds(pl.multiple_of(at, TILE_SIZE), TILE_SIZE)] = both.reshape(TILE_SIZE)

        loop(n // 8, body)
        for i, ref in outs:
            out_copy(ref, b, i, r, n).start()

    def wait_out(b, n):
        for i, ref in outs:
            out_copy(ref, b, i, 0, n).wait()

    load_round(0)

    mvwb[...] = jnp.zeros_like(mvwb)
    for i, ref in olds:
        mvwb[i, pl.ds(BPAD, BROWS - BPAD), :] = ends[pl.ds(i * (BROWS - BPAD), BROWS - BPAD), :]
    @pl.when(me < 15)
    def _():
        sized(me + 1, lambda n: ends_copy(n, me + 1).start())

    def stage(s):
        @when_round(s)
        def _():
            r, a, b = s, s % NACC, s % 2
            steps = turned(r)

            def sum_cores(rel):
                src, some = any_tiles(TILES), top(TILES)
                pltpu.make_async_copy(src, acc.at[a, some], own_sem.at[a, rel]).wait()
                remote(src, sib.at[b, some], sib_send.at[b], sib_recv.at[b, rel], mate).wait_recv()
                for t, n, first, base in SLOTS:
                    at = pl.ds(base + rel * n, n)
                    add_range(acc.at[a, at], sib.at[b, at], n)

            def send_half(rel):
                for t, n, first, base in SLOTS:
                    remote(acc.at[a, pl.ds(base + rel * n, n)], l1.at[r, pl.ds(base // 2 + (rel - 4) * n, n)],
                           rs_send.at[r, 0], rs_recv.at[r, t, 0], me + steps[t][0]).start()

            for rel in reversed(range(8)):
                sum_cores(rel)
                if 3 <= rel < 7:
                    send_half(rel + 1)

            @pl.when(r + 2 < ROUNDS)
            def _():
                pl.semaphore_signal(free_sem, inc=1, device_id=mesh_id(mate), device_id_type=MESH)

        nxt = s + 1

        @pl.when((nxt >= NACC) & (nxt < ROUNDS))
        def _():
            for j in range(3):
                rs_wait(nxt - NACC, j)

        @pl.when((nxt >= 2) & (nxt < ROUNDS))
        def _():
            remote(any_tiles(BLOCKS), sib.at[0], sib_send.at[nxt % 2], sib_recv.at[0, 0], mate).wait_send()
            pl.semaphore_wait(free_sem, 1)

        @pl.when(nxt < ROUNDS)
        def _():
            load_round(nxt)

        @pl.when(s == 2)
        def _():
            gb[...] = jnp.zeros_like(gb)
            for i in range(2):
                def spread(k, i=i):
                    row = BPAD + i * (BTAIL // LANES // 2) + k
                    gb[pl.ds(row, 1), :] = gvec[pl.ds(i, 1), pl.ds(pl.multiple_of(k * LANES, LANES), LANES)]

                loop(BTAIL // LANES // 2, spread)

        @pl.when(s == 2)
        def _():
            for i, ref in olds:
                old_copy(ref, 0, i, BROWS).start()

        @pl.when((s > 2) & (s < ROUNDS + 2))
        def _():
            for i, ref in olds:
                old_copy(ref, s - 2, i, 0).start()

        for j, land, out in ((1, l1, l2), (2, l2, l3)):
            @when_round(s - j)
            def _(j=j, land=land, out=out):
                r = s - j
                a = r % NACC
                keep = 4 >> j
                steps = turned(r)
                for t, n, first, base in SLOTS:
                    here = land.at[r, pl.ds(base >> j, 2 * keep * n)]
                    remote(here, here, rs_send.at[r, j - 1], rs_recv.at[r, t, j - 1], mate).wait_recv()
                    add_range(acc.at[a, pl.ds(base + keep * n, keep * n)],
                              land.at[r, pl.ds((base >> j) + keep * n, keep * n)], keep * n)
                for t, n, first, base in SLOTS:
                    remote(acc.at[a, pl.ds(base + keep * n, keep * n)], out.at[r, pl.ds(base >> (j + 1), keep * n)],
                           rs_send.at[r, j], rs_recv.at[r, t, j], me + steps[t][j]).start()
                for t, n, first, base in SLOTS:
                    add_range(acc.at[a, pl.ds(base, keep * n)], land.at[r, pl.ds(base >> j, keep * n)], keep * n)

        @when_round(s - 3)
        def _():
            r = s - 3
            a, b = r % NACC, r % 2

            @pl.when(r == 0)
            def _():
                old_rows(0, BROWS)

            @pl.when((r == 0) & (me > 0))
            def _():
                sized(me, lambda n: ends_copy(n, mate).wait_recv())

            @pl.when(r > 0)
            def _():
                old_rows(r, 0)

            @pl.when((r == 1) & (me > 0))
            def _():
                sized(me, lambda n: heads_copy(n, mate).wait_send())

            for i, ref in outs:
                mv[i, pl.ds(7, 1), :] = mv[i, pl.ds(ROWS + 7, 1), :]
            for t, n, first, base in SLOTS:
                here = l3.at[r, pl.ds(first, n)]
                remote(here, here, rs_send.at[r, 2], rs_recv.at[r, t, 2], mate).wait_recv()
            steps = turned(r)
            group = ROUNDS * me + r
            wide = (group >= TENSOR_GROUPS[1]) & (group < TENSOR_GROUPS[3])

            def adam_pass(stride):
                for t, n, first, base in SLOTS:
                    def body(u, first=first, base=base):
                        unit = first // 6 + u
                        if stride == 6:
                            row = unit * 48
                        else:
                            row = (unit // 4) * 192 + (unit % 4) * 6
                        for j in range(6):
                            old = []
                            for i, ref in olds:
                                at = row + j + BROWS - shift_rows
                                here = pltpu.roll(raw[i, pl.ds(at, 8, stride=stride), :], shift_lanes, 1)
                                prev = pltpu.roll(raw[i, pl.ds(at - 1, 8, stride=stride), :], shift_lanes, 1)
                                old.append(jnp.where(lane >= shift_lanes, here, prev))
                            tile = acc[a, base + u * 6 + j] + l3[r, unit * 6 + j]
                            new = adam_update(tile * (1.0 / 16.0), *old)
                            for i, ref in olds:
                                mv[i, pl.ds(row + j + 8, 8, stride=stride), :] = new[i]
                            wt[r, unit * 6 + j] = new[2].astype(jnp.bfloat16)

                    loop(n // 6, body)

            @pl.when(wide)
            def _():
                adam_pass(24)

            @pl.when(jnp.logical_not(wide))
            def _():
                adam_pass(6)

            for t, n, first, base in SLOTS:
                remote(wt.at[r, pl.ds(first, n)], block(me, r, first, n), ag_send.at[r, 0], ag_recv.at[r, t, 0],
                       me + steps[t][0]).start()
            mine = block(me, r, 0, TILES)
            remote(wt.at[r], mine, fw_send.at[r, 0], fw_recv.at[r, 0], mate).start()
            pltpu.make_async_copy(wt.at[r], mine, loc_sem.at[r]).start()

            @pl.when((r == 0) & (me > 0))
            def _():
                sized(me, lambda n: heads_copy(n, me - 1).start())

            @pl.when(r >= 2)
            def _():
                wait_out(b, ROWS)

            put_out(b, r, ROWS)

        @pl.when((s == ROUNDS + 3) & (me < 15))
        def _():
            sized(me + 1, lambda n: ends_copy(n, mate).wait_send())
            sized(me + 1, lambda n: heads_copy(n, mate).wait_recv())

        @pl.when(s == ROUNDS + 3)
        def _():
            wait_out(0, ROWS)
            for i, ref in outs:
                mv[i, pl.ds(7, 1), :] = mv[i, pl.ds(ROWS + 7, 1), :]
                mv[i, pl.ds(8, BROWS), :] = heads[i]
            put_out(0, ROUNDS, BROWS)

        for j in (1, 2, 3):
            @when_round(s - 3 - j)
            def _(j=j):
                r = s - 3 - j
                got = 1 << (j - 1)
                steps = turned(r)
                if j == 1:
                    pltpu.make_async_copy(wt.at[r], block(me, r, 0, TILES), loc_sem.at[r]).wait()
                for t, n, first, base in SLOTS:
                    part = wst.at[top(got * n)]
                    remote(part, part, ag_send.at[r, j - 1], ag_recv.at[r, t, j - 1], mate).wait_recv()
                    held = [me]
                    for step in steps[t][:j]:
                        held = held + [d + step for d in held]
                    if j < 3:
                        for d in held:
                            here = block(d, r, first, n)
                            remote(here, here, ag_send.at[r, j], ag_recv.at[r, t, j], me + steps[t][j]).start()
                    for d in held[got:]:
                        here = block(d, r, first, n)
                        remote(here, here, fw_send.at[r, j], fw_recv.at[r, j], mate).start()

        for j in range(9):
            @pl.when(s == j + 3)
            def _(j=j):
                if j > 0:
                    i = j - 1
                    land = bl.at[i] if i < 4 else wbl.at[i - 4]
                    remote(land, land, b_send.at[i], b_recv.at[i], mate).wait_recv()
                if j < 4:
                    src = gb
                    if j > 0:
                        src = bs.at[j - 1]
                        src[...] = (gb[...] if j == 1 else bs[j - 2]) + bl[j - 1]
                    remote(src, bl.at[j], b_send.at[j], b_recv.at[j], partners[j]).start()
                elif j < 8:
                    if j == 4:
                        new = adam_update((bs[2] + bl[3]) * (1.0 / 16.0), mvwb[0], mvwb[1], mvwb[2])
                        for i, ref in outs:
                            bout[i] = new[i]
                        keep = jnp.broadcast_to(me, (BROWS, LANES)) == 15
                        wbs[0] = jnp.where(keep, new[2], 0.0).astype(jnp.bfloat16)

                        @pl.when(me == 15)
                        def _():
                            for i, ref in outs:
                                heads[i, top(BROWS - BPAD), :] = bout[i, pl.ds(BPAD, BROWS - BPAD), :]
                    else:
                        wbs[j - 4] = wbs[j - 5] + wbl[j - 5]
                    remote(wbs.at[j - 4], wbl.at[j - 4], b_send.at[j], b_recv.at[j], partners[j - 4]).start()
                else:
                    wb_out[...] = wbs[3] + wbl[3]

    loop(STAGES, stage)

    for j in range(4):
        remote(gb, bl.at[j], b_send.at[j], b_recv.at[j], mate).wait_send()
        remote(wbs.at[j], wbl.at[j], b_send.at[4 + j], b_recv.at[4 + j], mate).wait_send()
    for b in range(2):
        remote(any_tiles(BLOCKS), sib.at[0], sib_send.at[b], sib_recv.at[0, 0], mate).wait_send()

    def drain(r):
        @pl.when(r >= ROUNDS - NACC)
        def _():
            for j in range(3):
                rs_wait(r, j)

        for j in range(3):
            part = wst.at[top(TILES << j)]
            remote(part, part, ag_send.at[r, j], ag_recv.at[r, 0, j], mate).wait_send()
        for j in range(4):
            part = wst.at[top(TILES << max(j - 1, 0))]
            remote(part, part, fw_send.at[r, j], fw_recv.at[r, j], mate).wait_send()
            remote(part, part, fw_send.at[r, j], fw_recv.at[r, j], mate).wait_recv()

    loop(ROUNDS, drain)
    wait_out(1, ROWS)
    wait_out(0, BROWS)


def comm_call(grads, gvec, olds, ends):
    any_spec = pl.BlockSpec(memory_space=pl.ANY)
    vmem_spec = pl.BlockSpec(memory_space=pltpu.VMEM)
    f32, bf16 = jnp.float32, jnp.bfloat16
    dma = pltpu.SemaphoreType.DMA
    flat = jax.ShapeDtypeStruct((OUT_ROWS * LANES,), f32)
    return pl.pallas_call(
        comm_kernel,
        name='adam_comm',
        out_shape=(
            jax.ShapeDtypeStruct((TENSOR_GROUPS[-1] * TILES,) + TILE, bf16), flat, flat, flat,
            jax.ShapeDtypeStruct((BROWS, LANES), bf16),
        ),
        in_specs=[any_spec] * 4 + [vmem_spec] + [any_spec] * 3 + [vmem_spec],
        out_specs=(any_spec,) * 4 + (vmem_spec,),
        scratch_shapes=[
            pltpu.VMEM((NACC, BLOCKS) + TILE, f32),
            pltpu.VMEM((2, BLOCKS) + TILE, f32),
            pltpu.VMEM((ROUNDS, BLOCKS // 2) + TILE, f32),
            pltpu.VMEM((ROUNDS, BLOCKS // 4) + TILE, f32),
            pltpu.VMEM((ROUNDS, TILES) + TILE, f32),
            pltpu.VMEM((2 * 3 * RAW_ROWS * LANES,), f32),
            pltpu.VMEM((3, RAW_ROWS, LANES), f32),
            pltpu.VMEM((3, ROWS + 8, LANES), f32),
            pltpu.VMEM((2 * 3 * ROWS * LANES,), f32),
            pltpu.VMEM((3, BROWS, LANES), f32),
            pltpu.VMEM((ROUNDS, TILES) + TILE, bf16),
            pltpu.VMEM((3, BROWS, LANES), f32),
            pltpu.VMEM((BROWS, LANES), f32),
            pltpu.VMEM((3, BROWS, LANES), f32),
            pltpu.VMEM((4, BROWS, LANES), f32),
            pltpu.VMEM((3, BROWS, LANES), f32),
            pltpu.VMEM((4, BROWS, LANES), bf16),
            pltpu.VMEM((4, BROWS, LANES), bf16),
            dma((NACC, 8)), dma((2,)), dma((2, 8)),
            dma((ROUNDS, 3)), dma((ROUNDS, 3, 3)),
            dma((ROUNDS, 3)), dma((ROUNDS, 3, 3)),
            dma((ROUNDS, 4)), dma((ROUNDS, 4)),
            dma((ROUNDS,)), dma((2,)), dma((2,)),
            dma((8,)), dma((8,)), dma((2,)), dma((2,)),
            pltpu.SemaphoreType.REGULAR,
        ],
        compiler_params=pltpu.CompilerParams(collective_id=0, has_side_effects=True, vmem_limit_bytes=67043328),
    )(*grads, gvec, *olds, ends)


RING = 16
AHEAD = 8
HALF = BLOCKS // 2
MOVES = TENSOR_GROUPS[-1] * TILES // HALF
CHIP_BLOCK = ROWS * LANES
CHIP_COUNT = 1968576
PER_PART = TENSOR_GROUPS[-1] // PARTS


def chip_group(pair, i):
    j = i - 2
    wide = 16 + 48 * (j // 6) + 24 * ((j % 6) // 3) + 3 * pair + j % 3
    first = jnp.where(i < 2, 1, 0)
    return first * (2 * pair + i) + (1 - first) * wide


def put_rows(rows, chip, first, count):
    def body(k):
        row = pl.multiple_of(first + k * 8, 8)
        flat = rows[pl.ds(row, 8), :].reshape(1, TILE_SIZE).astype(jnp.bfloat16)
        chip[:, pl.ds(pl.multiple_of(row * LANES, TILE_SIZE), TILE_SIZE)] = flat

    loop(count // 8, body, unroll=True)


def flatten_group(i, tiles, rows, chip, quarter):
    wide = (i >= 2) & (i < 14)

    def relay(stride):
        for u in range(4):
            row = quarter * 192 + u * (48 if stride == 6 else 6)
            for j in range(6):
                rows[pl.ds(row + j, 8, stride=stride), :] = tiles[quarter * 24 + u * 6 + j].astype(jnp.float32)

    @pl.when(wide)
    def _():
        relay(24)

    @pl.when(jnp.logical_not(wide))
    def _():
        relay(6)

    put_rows(rows, chip, quarter * 192, 192)


def unpack_kernel(wst, tail, m1, v1, w1, we, wa, wf, wh, chip, m2, v2, w2, buf, tiles, rows,
                  in_sem, out_sem, sem):
    me = device_number()
    pair = me // 2
    outs = (we, wa, wf, wh)
    i = pl.program_id(0)
    news = ((m1, m2), (v1, v2), (w1, w2))

    def some(k):
        return wst.at[pl.ds(k * HALF, HALF)]

    def start_in(k):
        slot = lax.rem(k, RING)
        pltpu.make_async_copy(some(k), buf.at[slot], in_sem.at[slot]).start()

    def wait_out(k):
        slot = lax.rem(k, RING)
        pltpu.make_async_copy(buf.at[slot], wa.at[top(HALF)], out_sem.at[slot]).wait()

    def part_copy(k):
        src = wst.at[pl.ds(chip_group(pair, k) * TILES, TILES)]
        return pltpu.make_async_copy(src, tiles.at[k % 2], sem.at[k % 2])

    for src, dst in news:
        dst[...] = src[...]

    @pl.when(i == 0)
    def _():
        part_copy(0).start()
        loop(AHEAD, start_in)

    def move(k):
        nxt = k + AHEAD

        @pl.when((nxt >= RING) & (nxt < MOVES))
        def _():
            wait_out(nxt)

        @pl.when(nxt < MOVES)
        def _():
            start_in(nxt)

        slot = lax.rem(k, RING)
        pltpu.make_async_copy(some(k), buf.at[slot], in_sem.at[slot]).wait()
        for ref, lo, hi in zip(outs, TENSOR_GROUPS, TENSOR_GROUPS[1:]):
            @pl.when((i * PER_PART >= lo) & (i * PER_PART < hi))
            def _(ref=ref, lo=lo):
                dst = ref.at[pl.ds(k * HALF - lo * TILES, HALF)]
                pltpu.make_async_copy(buf.at[slot], dst, out_sem.at[slot]).start()

    @pl.when(i + 1 < PARTS)
    def _():
        part_copy(i + 1).start()

    @pl.when(i < PARTS)
    def _():
        part_copy(i).wait()
        for k in range(2):
            move(2 * i + k)
            loop(2, lambda q: flatten_group(i, tiles.at[i % 2], rows, chip, 2 * k + q))

    @pl.when(i == PARTS)
    def _():
        put_rows(tail, chip, 0, 24)
        loop(RING, wait_out)


def unpack_call(wst, tail, new):
    any_spec = pl.BlockSpec(memory_space=pl.ANY)
    sizes = [hi - lo for lo, hi in zip(TENSOR_GROUPS, TENSOR_GROUPS[1:])]
    bf16 = jnp.bfloat16
    dma = pltpu.SemaphoreType.DMA
    return pl.pallas_call(
        unpack_kernel,
        name='unpack',
        grid=(PARTS + 1,),
        out_shape=tuple(jax.ShapeDtypeStruct((n * TILES,) + TILE, bf16) for n in sizes)
        + (jax.ShapeDtypeStruct((1, CHIP_COUNT), bf16),) + (jax.ShapeDtypeStruct((SHARD,), jnp.float32),) * 3,
        in_specs=[any_spec, pl.BlockSpec((24, LANES), lambda i: (0, 0))] + [pl.BlockSpec((NEW_ROWS * LANES,), lambda i: (i + 1,))] * 3,
        out_specs=(any_spec,) * 4 + (pl.BlockSpec((1, CHIP_BLOCK), lambda i: (0, i)),)
        + (pl.BlockSpec((NEW_ROWS * LANES,), lambda i: (i,)),) * 3,
        scratch_shapes=[
            pltpu.VMEM((RING, HALF) + TILE, bf16),
            pltpu.VMEM((2, TILES) + TILE, bf16),
            pltpu.VMEM((ROWS, LANES), jnp.float32),
            dma((RING,)), dma((RING,)), dma((2,)),
        ],
    )(wst, tail, *new)


def to_tiles(x):
    width = x.shape[-1] // LANES
    return x.reshape(-1, 8, width, LANES).transpose(0, 2, 1, 3).reshape(-1, 8, LANES)


def from_tiles(x, shape):
    width = shape[-1] // LANES
    return x.reshape(-1, width, 8, LANES).transpose(0, 2, 1, 3).reshape(shape)


def solution(mesh):
    def local_step(g_embed, g_attn, g_ffn_in, g_ffn_out, g_vec, m_shard, v_shard, w_shard):
        d = device_number()
        mats = (g_embed, g_attn, g_ffn_in, g_ffn_out)
        shapes = [g.shape[1:] for g in mats]
        grads = [to_tiles(g) for g in mats]
        shards = (m_shard, v_shard, w_shard)
        ends = jnp.concatenate([x[SHARD - BTAIL:] for x in shards]).reshape(-1, LANES)
        wst, *new, wb = comm_call(grads, g_vec[0], shards, ends)
        wb_vec = wb[BPAD:].reshape(g_vec.shape[1:])
        part = g_vec.shape[2] // 8
        tail = lax.dynamic_slice(wb_vec, (0, (d // 2) * part), (2, part)).reshape(-1).astype(jnp.float32)
        tail = jnp.pad(tail, (0, 24 * LANES - 2 * part)).reshape(24, LANES)
        *packed, chip, m_new, v_new, w_new = unpack_call(wst, tail, new)
        tensors = [from_tiles(x, shape) for x, shape in zip(packed, shapes)]
        return (m_new, v_new, w_new) + tuple(tensors) + (wb_vec, chip)

    return jax.shard_map(local_step, mesh=mesh, in_specs=(P(MESH_AXES),) * 8,
                         out_specs=(P(MESH_AXES),) * 3 + (P(),) * 5 + (P(MESH_AXES),), check_vma=False)
```
